32 devices in a mesh: dp: 16 (over z, y, core), level: 2 (over x).
Axes of the slice: x: 2, y: 2, z: 4, core: 2. Of those that a mesh axis runs over, the one named last changes fastest.
Arguments:
- token_ids: int32 [16, 2, 1536], P('dp', 'level'), may hold values from 0 to 1023
- decoded_mask: int32 [16, 2, 1536], P('dp', 'level'), may hold values 0 or 1
- levels_done: int32 [16], P('dp'), may hold values from 0 to 1
- code_tables: bfloat16 [2, 1024, 1024], P('level'), may hold values from -6 to 6
- mask_vectors: bfloat16 [2, 1024], P('level'), may hold values from -6 to 6
- w_qkv: bfloat16 [3, 1024, 1024], P(None, 'dp', 'level'), may hold values from -6 to 6
- w_out: bfloat16 [1024, 1024], P('level', 'dp'), may hold values from -0.1875 to 0.1875
- w_expand: bfloat16 [1024, 2048], P('dp'), may hold values from -0.1875 to 0.1875
- w_depth: bfloat16 [5, 1024], replicated, may hold values from -2.5 to 2.5
- w_project: bfloat16 [1024, 1024], P('dp'), may hold values from -0.1875 to 0.1875
- level_heads: bfloat16 [2, 1024, 1024], P('level'), may hold values from -0.1875 to 0.1875
Outputs:
- logits: bfloat16 [16, 2, 1536, 1024], P('dp', 'level')
The draws below stay inside these ranges and needn't reach their ends.
Inputs may be any that keep to these rules, and one draw needn't show every extreme that they name: `levels_done`: levels below it are fully decoded; the level equal to it is the one being decoded.
All inputs are finite; a program needn't handle non-finite values. No bound on the sum of `decoded_mask` on one device may be relied on, other than what follows from the above.
Results may differ from the reference program's by a relative error of at most 0.006.
Values may be sent and summed in bfloat16 or wider, within the bound.
A program may use at most 192 MiB of HBM per device.

```python
import jax
import jax.numpy as jnp
from jax import lax

D = 1024
HEADS = 16
VOCAB = 1024
FRAMES = 1536
KERNEL = 5
HEAD_DIM = 64
LEVELS = 2
CLIPS = 16


def draw_w_qkv(key, part):
    spread = D ** (-0.5)
    weights = jax.random.normal(jax.random.fold_in(key, 11), (3, D, D), jnp.float32) * spread
    weights = jnp.clip(weights, -6.0 * spread, 6.0 * spread)
    return jnp.clip(weights, -6.0, 6.0).astype(jnp.bfloat16)


def with_ends(values, key, low, top_value):
    longest = values.shape.index(max(values.shape))
    spots = []
    for shift in (0, 1):
        where = [jax.random.randint(jax.random.fold_in(key, axis), (), 0, length) for axis, length in enumerate(values.shape)]
        where[longest] = (where[longest] + shift) % values.shape[longest]
        spots.append(tuple(where))
    return values.at[spots[0]].set(low).at[spots[1]].set(top_value)


def block_scale(own_key, shape, split, low, top_value):
    gain = 1.0
    for dim, shards_of in split:
        steps = jax.random.uniform(jax.random.fold_in(jax.random.fold_in(own_key, 6), dim), (shards_of,), jnp.float32, low / len(split), top_value / len(split))
        gain = gain * jnp.repeat(jnp.exp(steps), shape[dim] // shards_of).reshape((-1,) + (1,) * (len(shape) - 1 - dim))
    return gain


def centred(stream_key, extent, width, bound, pieces=(), held_as=jnp.bfloat16):
    array = jax.random.normal(stream_key, extent, jnp.float32) * width
    if len(pieces) > 0:
        array = block_scale(stream_key, extent, pieces, -0.22, 0.18) * array
    return jnp.clip(array, min=-bound, max=bound).astype(held_as)


def setup_inputs(seed: int = 0) -> dict:
    streams_of = jax.random.split(jax.random.key(seed), 12)
    return {
        "token_ids": with_ends(jax.random.randint(streams_of[0], (CLIPS, LEVELS, FRAMES), 0, VOCAB), jax.random.fold_in(streams_of[0], 1), 0, VOCAB - 1).astype(jnp.int32),
        "decoded_mask": with_ends((jax.random.randint(streams_of[1], (CLIPS, LEVELS, FRAMES), 0, 2) < 1).astype(jnp.int32), jax.random.fold_in(streams_of[1], 1), 0, 1),
        "levels_done": with_ends(jax.random.randint(streams_of[2], (CLIPS,), 0, LEVELS), jax.random.fold_in(streams_of[2], 1), 0, LEVELS - 1).astype(jnp.int32),
        "code_tables": centred(streams_of[3], (LEVELS, VOCAB, D), 1.0, 6.0, ((0, 2),)),
        "mask_vectors": centred(streams_of[4], (LEVELS, D), 1.0, 6.0, ((0, 2),)),
        "w_qkv": draw_w_qkv(jax.random.fold_in(streams_of[11], 71), 0),
        "w_out": centred(streams_of[6], (D, D), D ** -0.5, 0.1875, ((0, 2), (1, 16))),
        "w_expand": centred(streams_of[7], (D, 2 * D), D ** -0.5, 0.1875, ((0, 16),)),
        "w_depth": centred(streams_of[8], (KERNEL, D), KERNEL ** -0.5, 2.5),
        "w_project": centred(streams_of[9], (D, D), D ** -0.5, 0.1875, ((0, 16),)),
        "level_heads": centred(streams_of[10], (LEVELS, D, VOCAB), D ** -0.5, 0.1875, ((0, 2),)),
    }


def layer_norm(values):
    centered = values - lax.optimization_barrier(jnp.mean(values, axis=-1, keepdims=True))
    variance = lax.optimization_barrier(jnp.mean(centered * centered, axis=-1, keepdims=True))
    return centered * lax.rsqrt(variance + 1e-05)

def clip_step(token_ids, decoded_mask, levels_done, code_tables, mask_vectors, w_qkv, w_out, w_expand, w_depth, w_project, level_heads):
    level_ids = jnp.arange(LEVELS, dtype=jnp.int32)[:, None]
    use_token = (level_ids < levels_done) | (level_ids == levels_done) & (decoded_mask == 1)
    picked = jax.vmap(lambda table_one, ids_one: jnp.take(table_one, ids_one, axis=0))(code_tables, token_ids.astype(jnp.int32)).astype(jnp.float32)
    terms = jnp.where(use_token[:, :, None], picked, mask_vectors.astype(jnp.float32)[:, None, :])
    embedded = lax.optimization_barrier(jnp.sum(terms, axis=0))
    normed = layer_norm(embedded).astype(jnp.bfloat16)
    queries = jnp.dot(normed, w_qkv[0], preferred_element_type=jnp.float32).astype(jnp.bfloat16)
    key_rows = jnp.dot(normed, w_qkv[1], preferred_element_type=jnp.float32).astype(jnp.bfloat16)
    value_rows = jnp.dot(normed, w_qkv[2], preferred_element_type=jnp.float32).astype(jnp.bfloat16)
    queries, key_rows, value_rows = lax.optimization_barrier((queries, key_rows, value_rows))
    query_three = queries.astype(jnp.float32).reshape(FRAMES, HEADS, HEAD_DIM)
    key_three = key_rows.astype(jnp.float32).reshape(FRAMES, HEADS, HEAD_DIM)
    value_three = value_rows.astype(jnp.float32).reshape(FRAMES, HEADS, HEAD_DIM)
    scores = jnp.einsum('qhd,khd->hqk', query_three, key_three) * HEAD_DIM ** (-0.5)
    row_max = lax.optimization_barrier(jnp.max(scores, axis=-1, keepdims=True))
    weights = jnp.exp(scores - row_max)
    weight_sum = lax.optimization_barrier(jnp.sum(weights, axis=-1))
    rounded = lax.optimization_barrier(weights.astype(jnp.bfloat16)).astype(jnp.float32)
    mixture = jnp.einsum('hqk,khd->qhd', rounded, value_three) / weight_sum.T[:, :, None]
    attended = mixture.reshape(FRAMES, D).astype(jnp.bfloat16)
    after_attn = embedded + jnp.dot(attended, w_out, preferred_element_type=jnp.float32)
    normed_two = layer_norm(after_attn).astype(jnp.bfloat16)
    gate_linear = jnp.dot(normed_two, w_expand, preferred_element_type=jnp.float32)
    gated = (gate_linear[:, :D] * jax.nn.sigmoid(gate_linear[:, D:])).astype(jnp.bfloat16)
    gated = lax.optimization_barrier(gated)
    half_width = KERNEL // 2
    padded = jnp.pad(gated.astype(jnp.float32), ((half_width, half_width), (0, 0)))
    conv = jnp.zeros((FRAMES, D), jnp.float32)
    for tap_index in range(KERNEL):
        conv = conv + padded[tap_index:tap_index + FRAMES] * w_depth[tap_index].astype(jnp.float32)
    activated = (conv * jax.nn.sigmoid(conv)).astype(jnp.bfloat16)
    after_conv = after_attn + jnp.dot(activated, w_project, preferred_element_type=jnp.float32)
    final_norm = layer_norm(after_conv).astype(jnp.bfloat16)
    return jax.vmap(lambda head_one: jnp.dot(final_norm, head_one, preferred_element_type=jnp.float32))(level_heads).astype(jnp.bfloat16)

def reference(token_ids, decoded_mask, levels_done, code_tables, mask_vectors, w_qkv, w_out, w_expand, w_depth, w_project, level_heads):

    def one_clip(clip_parts):
        return clip_step(clip_parts[0], clip_parts[1], clip_parts[2], code_tables, mask_vectors, w_qkv, w_out, w_expand, w_depth, w_project, level_heads)
    return lax.map(one_clip, (token_ids, decoded_mask, levels_done))
```

```python
import functools
import math

import jax
import jax.numpy as jnp
from jax import lax
from jax.experimental import pallas as pl
from jax.experimental.pallas import tpu as pltpu
from jax.sharding import PartitionSpec as P

HEADS = 16
CORES = 2
LANES = 128
MESH = pl.DeviceIdType.MESH


def layer_norm(values):
    centered = values - jnp.mean(values, axis=-1, keepdims=True)
    variance = jnp.mean(centered * centered, axis=-1, keepdims=True)
    return centered * lax.rsqrt(variance + 1e-05)


def dot_f32(left, right):
    return jnp.dot(left, right, preferred_element_type=jnp.float32)


def dot_nt(left, right):
    return lax.dot_general(left, right, (((1,), (1,)), ((), ())), preferred_element_type=jnp.float32)


def chip_at(position, chips):
    position = lax.rem(position + 2 * chips, chips)
    turned = position // (chips // 2)
    return (1 - turned) * 2 * position + turned * (2 * (chips - 1 - position) + 1)


def position_of(chip, chips):
    odd = lax.rem(chip, 2)
    return (1 - odd) * (chip // 2) + odd * (chips - 1 - chip // 2)


class Ring:
    def __init__(self, full, rows, chips, sems):
        self.full, self.rows, self.chips, self.half = full, rows, chips, chips // 2
        self.send, self.recv, self.sib_send, self.sib_recv = sems
        self.device = lax.axis_index("dp")
        self.core = lax.rem(self.device, CORES)
        self.position = position_of(self.device // CORES, chips)
        self.sent = []

    def block(self, position, core, part):
        row = (chip_at(position, self.chips) * CORES + core) * self.rows
        count = self.rows
        if part is not None:
            count = self.rows // 2
            row = row + part * count
        return self.full.at[:, pl.ds(pl.multiple_of(row, count), count), :]

    def part(self, way, step):
        return way if step == self.half - 1 else None

    def origin(self, way, step):
        return self.position - (1 + step) if way == 0 else self.position + (1 + step)

    def hop(self, way, step):
        towards = self.position + 1 if way == 0 else self.position - 1
        source = self.position - step if way == 0 else self.position + step
        ref = self.block(source, self.core, self.part(way, step))
        target = chip_at(towards, self.chips) * CORES + self.core
        return pltpu.make_async_remote_copy(
            src_ref=ref,
            dst_ref=ref,
            send_sem=self.send.at[way, step],
            recv_sem=self.recv.at[way, step],
            device_id={"dp": target},
            device_id_type=MESH,
        )

    def arrival(self, way, step):
        ref = self.block(self.origin(way, step), self.core, self.part(way, step))
        return pltpu.make_async_remote_copy(
            src_ref=ref,
            dst_ref=ref,
            send_sem=self.send.at[way, step],
            recv_sem=self.recv.at[way, step],
            device_id={"dp": self.device},
            device_id_type=MESH,
        )

    def share(self, way, step, core):
        position = self.position if step < 0 else self.origin(way, step)
        ref = self.block(position, core, None if step < 0 else self.part(way, step))
        sibling = self.device + 1 - 2 * self.core
        return pltpu.make_async_remote_copy(
            src_ref=ref,
            dst_ref=ref,
            send_sem=self.sib_send.at[way, step + 1],
            recv_sem=self.sib_recv.at[way, step + 1],
            device_id={"dp": sibling},
            device_id_type=MESH,
        )

    def start(self):
        for way in range(2):
            self.hop(way, 0).start()
        self.share(0, -1, self.core).start()

    def advance(self, step):
        for way in range(2):
            self.arrival(way, step).wait_recv()
            if step + 1 < self.half:
                self.hop(way, step + 1).start()
            self.share(way, step, self.core).start()

    def finish(self):
        for way in range(2):
            for step in range(self.half):
                self.hop(way, step).wait_send()
                self.share(way, step, self.core).wait_send()
                self.share(way, step, 1 - self.core).wait_recv()
        self.share(0, -1, self.core).wait_send()
        self.share(0, -1, 1 - self.core).wait_recv()


def front_kernel(
    levels, devices, frames, width,
    meta_ref, table_ref, qkv_ref, out_ref, expand_ref, project_ref,
    attended_ref, own_ref, rest_ref,
    metas, tables, proj, embedded, normed, keys, values, queries,
    local_sem, level_send, level_recv, table_send, table_recv,
    ring_a, ring_a_recv, sib_a, sib_a_recv, ring_b, ring_b_recv, sib_b, sib_b_recv,
):
    level = lax.axis_index("level")
    device = lax.axis_index("dp")
    core = lax.rem(device, CORES)
    sibling = device + 1 - 2 * core
    chips = devices // CORES
    rows = width // devices
    columns = width // levels
    local_rows = frames // levels
    codes = table_ref.shape[0]
    half_table = codes // CORES
    position = position_of(device // CORES, chips)

    barrier = pltpu.get_barrier_semaphore()
    for shift in range(1, levels):
        pl.semaphore_signal(barrier, inc=1, device_id={"level": lax.rem(level + shift, levels)}, device_id_type=MESH)
    for other in (
        sibling,
        chip_at(position + 1, chips) * CORES + core,
        chip_at(position - 1, chips) * CORES + core,
    ):
        pl.semaphore_signal(barrier, inc=1, device_id={"dp": other}, device_id_type=MESH)
    pl.semaphore_wait(barrier, levels + 2)

    own_rows = pl.ds(pl.multiple_of(device * rows, rows), rows)
    own_columns = pl.ds(pl.multiple_of(level * columns, columns), columns)
    places = (
        (qkv_ref, proj.at[:, own_rows, own_columns]),
        (out_ref, rest_ref.at[pl.ds(0, 1), own_rows, own_columns]),
        (meta_ref, metas.at[level]),
    )
    half_rows = pl.ds(pl.multiple_of(core * half_table, half_table), half_table)
    other_half = pl.ds(pl.multiple_of((1 - core) * half_table, half_table), half_table)

    def over_level(kind, shift):
        source, place = places[kind]
        return pltpu.make_async_remote_copy(
            src_ref=source, dst_ref=place,
            send_sem=level_send.at[kind, shift], recv_sem=level_recv.at[kind, shift],
            device_id={"level": lax.rem(level + shift, levels)}, device_id_type=MESH,
        )

    def from_level(kind, shift):
        sender = lax.rem(level + levels - shift, levels)
        sender_columns = pl.ds(pl.multiple_of(sender * columns, columns), columns)
        source = places[kind][0]
        place = (
            proj.at[:, own_rows, sender_columns],
            rest_ref.at[pl.ds(0, 1), own_rows, sender_columns],
            metas.at[sender],
        )[kind]
        return pltpu.make_async_remote_copy(
            src_ref=source, dst_ref=place,
            send_sem=level_send.at[kind, shift], recv_sem=level_recv.at[kind, shift],
            device_id={"level": sender}, device_id_type=MESH,
        )

    def table_out(shift):
        return pltpu.make_async_remote_copy(
            src_ref=table_ref.at[half_rows], dst_ref=tables.at[level, half_rows],
            send_sem=table_send.at[0, shift], recv_sem=table_recv.at[0, shift],
            device_id={"level": lax.rem(level + shift, levels)}, device_id_type=MESH,
        )

    def table_at(shift, span, kind):
        sender = lax.rem(level + levels - shift, levels)
        place = tables.at[sender, span]
        return pltpu.make_async_remote_copy(
            src_ref=place, dst_ref=place,
            send_sem=table_send.at[kind, shift], recv_sem=table_recv.at[kind, shift],
            device_id={"dp": sibling}, device_id_type=MESH,
        )

    locals_ = [
        pltpu.make_async_copy(source, place, local_sem.at[i]) for i, (source, place) in enumerate(places)
    ] + [
        pltpu.make_async_copy(table_ref, tables.at[level], local_sem.at[3]),
        pltpu.make_async_copy(expand_ref.at[:, pl.ds(0, width)], rest_ref.at[1, own_rows, :], local_sem.at[4]),
        pltpu.make_async_copy(expand_ref.at[:, pl.ds(width, width)], rest_ref.at[2, own_rows, :], local_sem.at[5]),
        pltpu.make_async_copy(project_ref, rest_ref.at[3, own_rows, :], local_sem.at[6]),
    ]
    for kind in (0, 2):
        for shift in range(1, levels):
            over_level(kind, shift).start()
    for copy in locals_:
        copy.start()
    for shift in range(1, levels):
        table_out(shift).start()
    for shift in range(1, levels):
        over_level(1, shift).start()

    first = Ring(proj, rows, chips, (ring_a, ring_a_recv, sib_a, sib_a_recv))
    second = Ring(rest_ref, rows, chips, (ring_b, ring_b_recv, sib_b, sib_b_recv))

    for copy in locals_:
        copy.wait()
    for shift in range(1, levels):
        from_level(0, shift).wait_recv()
    first.start()
    for step in range(chips // 2 - 1):
        first.advance(step)
    for shift in range(1, levels):
        from_level(2, shift).wait_recv()
        table_at(shift, half_rows, 0).wait_recv()
        table_at(shift, half_rows, 1).start()
    for shift in range(1, levels):
        table_at(shift, half_rows, 1).wait_send()
        table_at(shift, other_half, 1).wait_recv()
        from_level(1, shift).wait_recv()
    first.advance(chips // 2 - 1)
    second.start()

    tile = 2 * LANES
    @pl.loop(0, frames // tile)
    def _(step):
        span = pl.ds(pl.multiple_of(step * tile, tile), tile)
        total = jnp.zeros((tile, width), jnp.float32)
        lane = lax.broadcasted_iota(jnp.int32, (tile, LANES), 1).astype(jnp.float32)
        for row in range(levels):
            ids = jnp.concatenate(
                [
                    jnp.broadcast_to(
                        metas[row, 0:1, pl.ds(pl.multiple_of(step * tile + piece * LANES, LANES), LANES)],
                        (LANES, LANES),
                    ).T
                    for piece in range(tile // LANES)
                ],
                axis=0,
            )
            onehot = jnp.concatenate(
                [
                    jnp.where(ids == lane + float(base), 1.0, 0.0).astype(jnp.bfloat16)
                    for base in range(0, codes, LANES)
                ],
                axis=1,
            )
            picked = dot_f32(onehot, tables[row])
            fill = metas[row, 8:9, 0:width]
            total = total + jnp.where(ids[:, 0:1] < 0.0, fill, picked)
        embedded[span, :] = total
        normed[span, :] = layer_norm(total).astype(jnp.bfloat16)

    own_frames = pl.ds(pl.multiple_of(level * local_rows, local_rows), local_rows)
    own_ref[...] = embedded[own_frames, :]
    first.finish()

    @pl.loop(0, frames // tile)
    def _(step):
        span = pl.ds(pl.multiple_of(step * tile, tile), tile)
        keys[span, :] = dot_f32(normed[span, :], proj[1]).astype(jnp.bfloat16)
        values[span, :] = dot_f32(normed[span, :], proj[2]).astype(jnp.bfloat16)

    head_dim = width // HEADS
    scale = head_dim ** (-0.5)
    block = math.gcd(local_rows, tile)

    @pl.loop(0, local_rows // block)
    def _(step):
        begin = pl.multiple_of(level * local_rows + step * block, block)
        to = pl.ds(pl.multiple_of(step * block, block), block)
        found = dot_f32(normed[pl.ds(begin, block), :], proj[0]).astype(jnp.bfloat16)
        queries[to, :] = found * jnp.asarray(scale, jnp.bfloat16)

    blocks = local_rows // block
    turns = (width // LANES) * blocks
    hops = chips // 2

    @pl.loop(0, turns)
    def _(turn):
        for step in range(hops):
            @pl.when(turn == (step + 1) * turns // hops - 1)
            def _():
                second.advance(step)

        pair = turn // blocks
        to = pl.ds(pl.multiple_of(lax.rem(turn, blocks) * block, block), block)
        across = pl.ds(pl.multiple_of(pair * LANES, LANES), LANES)
        query = queries[to, across]
        key = keys[:, across]
        value = values[:, across]
        lower = lax.broadcasted_iota(jnp.int32, (block, LANES), 1) < head_dim
        lower_value = lax.broadcasted_iota(jnp.int32, (frames, LANES), 1) < head_dim
        one = jnp.ones_like(value)
        zero = jnp.zeros_like(query)
        sums = []
        for low in (True, False):
            masked = jnp.where(lower, query, zero) if low else jnp.where(lower, zero, query)
            scores = dot_nt(masked, key)
            weights = jnp.exp(scores - jnp.max(scores, axis=-1, keepdims=True)).astype(jnp.bfloat16)
            extended = jnp.where(lower_value, value, one) if low else jnp.where(lower_value, one, value)
            sums.append(dot_f32(weights, extended))
        above = jnp.where(lower, sums[0], sums[1])
        below = pltpu.roll(jnp.where(lower, sums[1], sums[0]), head_dim, 1)
        attended_ref[to, across] = (above / below).astype(jnp.bfloat16)

    second.finish()
    for shift in range(1, levels):
        table_out(shift).wait_send()
        for kind in range(3):
            over_level(kind, shift).wait_send()


def front(levels, devices, ids, fill, table, w_qkv, w_out_t, w_expand, w_project):
    frames, width = ids.shape[0], table.shape[1]
    chips = devices // CORES
    local_rows = frames // levels
    span = max(frames, width)
    meta = jnp.concatenate(
        [
            jnp.broadcast_to(jnp.pad(ids, (0, span - frames)), (8, span)),
            jnp.broadcast_to(jnp.pad(fill, (0, span - width)), (8, span)),
        ]
    )
    vmem = pl.BlockSpec(memory_space=pltpu.VMEM)
    anywhere = pl.BlockSpec(memory_space=pl.ANY)
    dma = pltpu.SemaphoreType.DMA
    half = chips // 2
    bf16, f32 = jnp.bfloat16, jnp.float32
    return pl.pallas_call(
        functools.partial(front_kernel, levels, devices, frames, width),
        out_shape=(
            jax.ShapeDtypeStruct((local_rows, width), bf16),
            jax.ShapeDtypeStruct((local_rows, width), f32),
            jax.ShapeDtypeStruct((4, width, width), bf16),
        ),
        in_specs=[anywhere] * 6,
        out_specs=(vmem, vmem, vmem),
        scratch_shapes=[
            pltpu.VMEM((levels,) + meta.shape, f32),
            pltpu.VMEM((levels,) + table.shape, bf16),
            pltpu.VMEM((3, width, width), bf16),
            pltpu.VMEM((frames, width), f32),
            pltpu.VMEM((frames, width), bf16),
            pltpu.VMEM((frames, width), bf16),
            pltpu.VMEM((frames, width), bf16),
            pltpu.VMEM((local_rows, width), bf16),
            dma((7,)),
            dma((3, levels)), dma((3, levels)), dma((2, levels)), dma((2, levels)),
        ]
        + [dma((2, half)), dma((2, half)), dma((2, half + 1)), dma((2, half + 1))] * 2,
        compiler_params=pltpu.CompilerParams(
            collective_id=0, has_side_effects=True, vmem_limit_bytes=64000 * 1024
        ),
    )(meta, table, w_qkv, w_out_t, w_expand, w_project)


def with_halo(x, sides, width):
    for axis, dim in sides:
        devices, length = (lax.axis_size(axis), x.shape[dim])
        up = [(i, (i + 1) % devices) for i in range(devices - 1)]
        down = [(j, i) for i, j in up]
        last = lax.slice_in_dim(x, length - width, length, axis=dim)
        leading = lax.slice_in_dim(x, 0, width, axis=dim)
        before = lax.ppermute(last, axis, up)
        after = lax.ppermute(leading, axis, down)
        x = jnp.concatenate([before, x, after], axis=dim)
    return x


def body(
    token_ids,
    decoded_mask,
    levels_done,
    code_tables,
    mask_vectors,
    w_qkv,
    w_out,
    w_expand,
    w_depth,
    w_project,
    level_heads,
):
    frames = token_ids.shape[2]
    groups = lax.axis_size("level")
    level_index = lax.axis_index("level")
    local_rows = frames // groups
    done_count = levels_done[0]
    use_token = (level_index < done_count) | ((level_index == done_count) & (decoded_mask[0, 0] == 1))
    ids = jnp.where(use_token, token_ids[0, 0], -1).astype(jnp.float32)
    attended, own_rows, rest = front(
        groups, lax.axis_size("dp"), ids, mask_vectors[0].astype(jnp.float32), code_tables[0],
        w_qkv, w_out.T[None], w_expand, w_project,
    )
    after_attn = own_rows + dot_nt(attended, rest[0])
    normed_two = layer_norm(after_attn).astype(jnp.bfloat16)
    gated = (
        dot_f32(normed_two, rest[1]) * jax.nn.sigmoid(dot_f32(normed_two, rest[2]))
    ).astype(jnp.bfloat16)
    half_width = w_depth.shape[0] // 2
    padded = with_halo(gated, (("level", 0),), half_width)
    conv = jnp.zeros(gated.shape, jnp.float32)
    for tap_index in range(w_depth.shape[0]):
        conv = conv + padded[tap_index : tap_index + local_rows].astype(jnp.float32) * w_depth[
            tap_index
        ].astype(jnp.float32)
    activated = (conv * jax.nn.sigmoid(conv)).astype(jnp.bfloat16)
    after_conv = after_attn + dot_f32(activated, rest[3])
    final_norm = layer_norm(after_conv).astype(jnp.bfloat16)
    own_head = level_heads[0]
    logits = jnp.zeros((frames, own_head.shape[1]), jnp.bfloat16)
    pieces = [final_norm]
    for shift in range(1, groups):
        pieces.append(
            lax.ppermute(final_norm, "level", [(i, (i + shift) % groups) for i in range(groups)])
        )
    for shift, piece in enumerate(pieces):
        origin = (level_index + groups - shift) % groups
        logits = lax.dynamic_update_slice_in_dim(
            logits, dot_f32(piece, own_head).astype(jnp.bfloat16), origin * local_rows, axis=0
        )
    return logits[None, None]


def solution(mesh):
    return jax.shard_map(
        body,
        mesh=mesh,
        in_specs=(
            P("dp", "level", None),
            P("dp", "level", None),
            P("dp"),
            P("level", None, None),
            P("level", None),
            P(None, "dp", "level"),
            P("level", "dp"),
            P("dp", None),
            P(),
            P("dp", None),
            P("level", None, None),
        ),
        out_specs=P("dp", "level", None, None),
        check_vma=False,
    )
```

```python
import functools
import math

import jax
import jax.numpy as jnp
from jax import lax
from jax.experimental import pallas as pl
from jax.experimental.pallas import tpu as pltpu
from jax.sharding import PartitionSpec as P

HEADS = 16
CORES = 2
LANES = 128
HALO = 16
MESH = pl.DeviceIdType.MESH


def layer_norm(values):
    centered = values - jnp.mean(values, axis=-1, keepdims=True)
    variance = jnp.mean(centered * centered, axis=-1, keepdims=True)
    return centered * lax.rsqrt(variance + 1e-05)


def dot_f32(left, right):
    return jnp.dot(left, right, preferred_element_type=jnp.float32)


def dot_nt(left, right):
    return lax.dot_general(left, right, (((1,), (1,)), ((), ())), preferred_element_type=jnp.float32)


def chip_at(position, chips):
    position = lax.rem(position + 2 * chips, chips)
    turned = position // (chips // 2)
    return (1 - turned) * 2 * position + turned * (2 * (chips - 1 - position) + 1)


def position_of(chip, chips):
    odd = lax.rem(chip, 2)
    return (1 - odd) * (chip // 2) + odd * (chips - 1 - chip // 2)


class Ring:
    def __init__(self, full, rows, chips, sems):
        self.full, self.rows, self.chips, self.half = full, rows, chips, chips // 2
        self.send, self.recv, self.sib_send, self.sib_recv = sems
        self.device = lax.axis_index("dp")
        self.core = lax.rem(self.device, CORES)
        self.position = position_of(self.device // CORES, chips)
        self.sent = []

    def block(self, position, core, part):
        row = (chip_at(position, self.chips) * CORES + core) * self.rows
        count = self.rows
        if part is not None:
            count = self.rows // 2
            row = row + part * count
        return self.full.at[:, pl.ds(pl.multiple_of(row, count), count), :]

    def part(self, way, step):
        return way if step == self.half - 1 else None

    def origin(self, way, step):
        return self.position - (1 + step) if way == 0 else self.position + (1 + step)

    def hop(self, way, step):
        towards = self.position + 1 if way == 0 else self.position - 1
        source = self.position - step if way == 0 else self.position + step
        ref = self.block(source, self.core, self.part(way, step))
        target = chip_at(towards, self.chips) * CORES + self.core
        return pltpu.make_async_remote_copy(
            src_ref=ref,
            dst_ref=ref,
            send_sem=self.send.at[way, step],
            recv_sem=self.recv.at[way, step],
            device_id={"dp": target},
            device_id_type=MESH,
        )

    def arrival(self, way, step):
        ref = self.block(self.origin(way, step), self.core, self.part(way, step))
        return pltpu.make_async_remote_copy(
            src_ref=ref,
            dst_ref=ref,
            send_sem=self.send.at[way, step],
            recv_sem=self.recv.at[way, step],
            device_id={"dp": self.device},
            device_id_type=MESH,
        )

    def share(self, way, step, core):
        position = self.position if step < 0 else self.origin(way, step)
        ref = self.block(position, core, None if step < 0 else self.part(way, step))
        sibling = self.device + 1 - 2 * self.core
        return pltpu.make_async_remote_copy(
            src_ref=ref,
            dst_ref=ref,
            send_sem=self.sib_send.at[way, step + 1],
            recv_sem=self.sib_recv.at[way, step + 1],
            device_id={"dp": sibling},
            device_id_type=MESH,
        )

    def start(self):
        for way in range(2):
            self.hop(way, 0).start()
        self.share(0, -1, self.core).start()

    def advance(self, step):
        for way in range(2):
            self.arrival(way, step).wait_recv()
            if step + 1 < self.half:
                self.hop(way, step + 1).start()
            self.share(way, step, self.core).start()

    def finish(self):
        for way in range(2):
            for step in range(self.half):
                self.hop(way, step).wait_send()
                self.share(way, step, self.core).wait_send()
                self.share(way, step, 1 - self.core).wait_recv()
        self.share(0, -1, self.core).wait_send()
        self.share(0, -1, 1 - self.core).wait_recv()


def step_kernel(
    levels, devices, frames, width,
    meta_ref, table_ref, qkv_ref, out_ref, expand_ref, project_ref, head_ref, depth_ref,
    logits_ref,
    metas, tables, proj, rest_ref, embedded, normed, keys, values, queries,
    attended, gated, final, head,
    halo_send, halo_recv, final_send, final_recv,
    local_sem, level_send, level_recv, table_send, table_recv,
    ring_a, ring_a_recv, sib_a, sib_a_recv, ring_b, ring_b_recv, sib_b, sib_b_recv,
):
    level = lax.axis_index("level")
    device = lax.axis_index("dp")
    core = lax.rem(device, CORES)
    sibling = device + 1 - 2 * core
    chips = devices // CORES
    rows = width // devices
    columns = width // levels
    local_rows = frames // levels
    codes = table_ref.shape[0]
    half_table = codes // CORES
    position = position_of(device // CORES, chips)

    barrier = pltpu.get_barrier_semaphore()
    for shift in range(1, levels):
        pl.semaphore_signal(barrier, inc=1, device_id={"level": lax.rem(level + shift, levels)}, device_id_type=MESH)
    for other in (
        sibling,
        chip_at(position + 1, chips) * CORES + core,
        chip_at(position - 1, chips) * CORES + core,
    ):
        pl.semaphore_signal(barrier, inc=1, device_id={"dp": other}, device_id_type=MESH)
    pl.semaphore_wait(barrier, levels + 2)

    own_rows = pl.ds(pl.multiple_of(device * rows, rows), rows)
    own_columns = pl.ds(pl.multiple_of(level * columns, columns), columns)
    places = (
        (qkv_ref, proj.at[:, own_rows, own_columns]),
        (out_ref, rest_ref.at[pl.ds(0, 1), own_rows, own_columns]),
        (meta_ref, metas.at[level]),
    )
    half_rows = pl.ds(pl.multiple_of(core * half_table, half_table), half_table)
    other_half = pl.ds(pl.multiple_of((1 - core) * half_table, half_table), half_table)

    def over_level(kind, shift):
        source, place = places[kind]
        return pltpu.make_async_remote_copy(
            src_ref=source, dst_ref=place,
            send_sem=level_send.at[kind, shift], recv_sem=level_recv.at[kind, shift],
            device_id={"level": lax.rem(level + shift, levels)}, device_id_type=MESH,
        )

    def from_level(kind, shift):
        sender = lax.rem(level + levels - shift, levels)
        sender_columns = pl.ds(pl.multiple_of(sender * columns, columns), columns)
        source = places[kind][0]
        place = (
            proj.at[:, own_rows, sender_columns],
            rest_ref.at[pl.ds(0, 1), own_rows, sender_columns],
            metas.at[sender],
        )[kind]
        return pltpu.make_async_remote_copy(
            src_ref=source, dst_ref=place,
            send_sem=level_send.at[kind, shift], recv_sem=level_recv.at[kind, shift],
            device_id={"level": sender}, device_id_type=MESH,
        )

    def table_out(shift):
        return pltpu.make_async_remote_copy(
            src_ref=table_ref.at[half_rows], dst_ref=tables.at[level, half_rows],
            send_sem=table_send.at[0, shift], recv_sem=table_recv.at[0, shift],
            device_id={"level": lax.rem(level + shift, levels)}, device_id_type=MESH,
        )

    def table_at(shift, span, kind):
        sender = lax.rem(level + levels - shift, levels)
        place = tables.at[sender, span]
        return pltpu.make_async_remote_copy(
            src_ref=place, dst_ref=place,
            send_sem=table_send.at[kind, shift], recv_sem=table_recv.at[kind, shift],
            device_id={"dp": sibling}, device_id_type=MESH,
        )

    locals_ = [
        pltpu.make_async_copy(source, place, local_sem.at[i]) for i, (source, place) in enumerate(places)
    ] + [
        pltpu.make_async_copy(table_ref, tables.at[level], local_sem.at[3]),
        pltpu.make_async_copy(expand_ref.at[:, pl.ds(0, width)], rest_ref.at[1, own_rows, :], local_sem.at[4]),
        pltpu.make_async_copy(expand_ref.at[:, pl.ds(width, width)], rest_ref.at[2, own_rows, :], local_sem.at[5]),
        pltpu.make_async_copy(project_ref, rest_ref.at[3, own_rows, :], local_sem.at[6]),
    ]
    head_copy = pltpu.make_async_copy(head_ref, head, local_sem.at[7])
    for kind in (0, 2):
        for shift in range(1, levels):
            over_level(kind, shift).start()
    for copy in locals_:
        copy.start()
    for shift in range(1, levels):
        table_out(shift).start()
    for shift in range(1, levels):
        over_level(1, shift).start()
    head_copy.start()

    first = Ring(proj, rows, chips, (ring_a, ring_a_recv, sib_a, sib_a_recv))
    second = Ring(rest_ref, rows, chips, (ring_b, ring_b_recv, sib_b, sib_b_recv))

    for copy in locals_:
        copy.wait()
    for shift in range(1, levels):
        from_level(0, shift).wait_recv()
    first.start()
    hops = chips // 2
    early = max(hops - 2, 0)
    for step in range(early):
        first.advance(step)
    for shift in range(1, levels):
        from_level(2, shift).wait_recv()
        table_at(shift, half_rows, 0).wait_recv()
        table_at(shift, half_rows, 1).start()
    for shift in range(1, levels):
        table_at(shift, half_rows, 1).wait_send()
        table_at(shift, other_half, 1).wait_recv()
        from_level(1, shift).wait_recv()

    tile = 2 * LANES
    @pl.loop(0, frames // tile)
    def _(step):
        for hop in range(early, hops):
            @pl.when(step == (hop - early) * (frames // tile) // 2)
            def _():
                first.advance(hop)
                if hop == hops - 1:
                    second.start()

        span = pl.ds(pl.multiple_of(step * tile, tile), tile)
        total = jnp.zeros((tile, width), jnp.float32)
        lane = lax.broadcasted_iota(jnp.int32, (tile, LANES), 1).astype(jnp.float32)
        for row in range(levels):
            ids = jnp.concatenate(
                [
                    jnp.broadcast_to(
                        metas[row, 0:1, pl.ds(pl.multiple_of(step * tile + piece * LANES, LANES), LANES)],
                        (LANES, LANES),
                    ).T
                    for piece in range(tile // LANES)
                ],
                axis=0,
            )
            onehot = jnp.concatenate(
                [
                    jnp.where(ids == lane + float(base), 1.0, 0.0).astype(jnp.bfloat16)
                    for base in range(0, codes, LANES)
                ],
                axis=1,
            )
            picked = dot_f32(onehot, tables[row])
            fill = metas[row, 8:9, 0:width]
            total = total + jnp.where(ids[:, 0:1] < 0.0, fill, picked)
        embedded[span, :] = total
        normed[span, :] = layer_norm(total).astype(jnp.bfloat16)

    first.finish()

    @pl.loop(0, frames // tile)
    def _(step):
        span = pl.ds(pl.multiple_of(step * tile, tile), tile)
        keys[span, :] = dot_f32(normed[span, :], proj[1]).astype(jnp.bfloat16)
        values[span, :] = dot_f32(normed[span, :], proj[2]).astype(jnp.bfloat16)

    head_dim = width // HEADS
    scale = head_dim ** (-0.5)
    block = math.gcd(local_rows, tile)

    @pl.loop(0, local_rows // block)
    def _(step):
        begin = pl.multiple_of(level * local_rows + step * block, block)
        to = pl.ds(pl.multiple_of(step * block, block), block)
        found = dot_f32(normed[pl.ds(begin, block), :], proj[0]).astype(jnp.bfloat16)
        queries[to, :] = found * jnp.asarray(scale, jnp.bfloat16)

    blocks = local_rows // block
    pairs = width // LANES
    turns = pairs * min(2, blocks)
    pad = HALO
    taps = depth_ref.shape[0]
    odd_level = lax.rem(level, 2)

    def chunk_of(owner, order):
        odd = lax.rem(owner, 2)
        return odd * order + (1 - odd) * (blocks - 1 - order)

    def local_span(order):
        return pl.ds(pl.multiple_of(chunk_of(level, order) * block, block), block)

    def clip_span(owner, order):
        start = owner * local_rows + chunk_of(owner, order) * block
        return pl.ds(pl.multiple_of(start, block), block)

    def halo(way):
        source = (pl.ds(local_rows, pad), pl.ds(pad, pad))[way]
        place = (pl.ds(0, pad), pl.ds(pad + local_rows, pad))[way]
        target = level + 1 if way == 0 else level - 1
        return pltpu.make_async_remote_copy(
            src_ref=gated.at[source], dst_ref=gated.at[place],
            send_sem=halo_send.at[way], recv_sem=halo_recv.at[way],
            device_id={"level": target}, device_id_type=MESH,
        )

    has = (level < levels - 1, level > 0)

    def halo_start(way):
        pl.when(has[way])(lambda: halo(way).start())

    def halo_wait(way):
        pl.when(has[1 - way])(lambda: halo(way).wait_recv())

    def spread(owner, order, shift, target):
        return pltpu.make_async_remote_copy(
            src_ref=final.at[clip_span(owner, order)], dst_ref=final.at[clip_span(owner, order)],
            send_sem=final_send.at[order, shift], recv_sem=final_recv.at[order, shift],
            device_id={"level": target}, device_id_type=MESH,
        )

    @pl.when(level == 0)
    def _():
        gated[pl.ds(0, pad), :] = jnp.zeros((pad, width), jnp.bfloat16)

    @pl.when(level == levels - 1)
    def _():
        gated[pl.ds(pad + local_rows, pad), :] = jnp.zeros((pad, width), jnp.bfloat16)

    def attend(order):
        to = local_span(order)

        @pl.loop(0, pairs)
        def _(pair):
            turn = order * pairs + pair
            for step in range(hops):
                @pl.when(turn == (step + 1) * turns // hops - 1)
                def _():
                    second.advance(step)

            across = pl.ds(pl.multiple_of(pair * LANES, LANES), LANES)
            query = queries[to, across]
            key = keys[:, across]
            value = values[:, across]
            lower = lax.broadcasted_iota(jnp.int32, (block, LANES), 1) < head_dim
            lower_value = lax.broadcasted_iota(jnp.int32, (frames, LANES), 1) < head_dim
            one = jnp.ones_like(value)
            zero = jnp.zeros_like(query)
            sums = []
            for low in (True, False):
                masked = jnp.where(lower, query, zero) if low else jnp.where(lower, zero, query)
                scores = dot_nt(masked, key)
                weights = jnp.exp(scores - jnp.max(scores, axis=-1, keepdims=True)).astype(jnp.bfloat16)
                extended = jnp.where(lower_value, value, one) if low else jnp.where(lower_value, one, value)
                sums.append(dot_f32(weights, extended))
            above = jnp.where(lower, sums[0], sums[1])
            below = pltpu.roll(jnp.where(lower, sums[1], sums[0]), head_dim, 1)
            attended[to, across] = (above / below).astype(jnp.bfloat16)

    def gate(order):
        own = clip_span(level, order)
        after_attn = embedded[own, :] + dot_nt(attended[local_span(order), :], rest_ref[0])
        embedded[own, :] = after_attn
        normed_two = layer_norm(after_attn).astype(jnp.bfloat16)
        mixed = dot_f32(normed_two, rest_ref[1]) * jax.nn.sigmoid(dot_f32(normed_two, rest_ref[2]))
        start = pl.multiple_of(pad + chunk_of(level, order) * block, pad)
        gated[pl.ds(start, block), :] = mixed.astype(jnp.bfloat16)

    def convolve(order):
        own = clip_span(level, order)
        start = pl.multiple_of(chunk_of(level, order) * block, block)
        window = gated[pl.ds(start, block + 2 * pad), :].astype(jnp.float32)
        conv = jnp.zeros((block, width), jnp.float32)
        for tap in range(taps):
            first_row = pad - taps // 2 + tap
            conv = conv + window[first_row : first_row + block] * depth_ref[tap : tap + 1, :]
        activated = (conv * jax.nn.sigmoid(conv)).astype(jnp.bfloat16)
        after_conv = embedded[own, :] + dot_f32(activated, rest_ref[3])
        final[own, :] = layer_norm(after_conv).astype(jnp.bfloat16)

    def score(owner, order):
        span = clip_span(owner, order)
        logits_ref[span, :] = dot_f32(final[span, :], head[...]).astype(jnp.bfloat16)

    @pl.loop(0, blocks + 2)
    def _(stage):
        pl.when(stage < blocks)(lambda: attend(stage))

        @pl.when(stage == 1)
        def _():
            if turns < hops:
                for step in range(hops):
                    if (step + 1) * turns // hops == 0:
                        second.advance(step)
            second.finish()
            head_copy.wait()

        @pl.when((stage >= 1) & (stage <= blocks))
        def _():
            gate(stage - 1)

        @pl.when((stage == 1) & (odd_level == 0))
        def _():
            halo_start(0)

        @pl.when((stage == 1) & (odd_level == 1))
        def _():
            halo_start(1)

        @pl.when((stage == blocks) & (odd_level == 0))
        def _():
            halo_start(1)

        @pl.when((stage == blocks) & (odd_level == 1))
        def _():
            halo_start(0)

        @pl.when((stage == 2) & (odd_level == 0))
        def _():
            halo_wait(1)

        @pl.when((stage == 2) & (odd_level == 1))
        def _():
            halo_wait(0)

        @pl.when((stage == blocks + 1) & (odd_level == 0))
        def _():
            halo_wait(0)

        @pl.when((stage == blocks + 1) & (odd_level == 1))
        def _():
            halo_wait(1)

        @pl.when(stage >= 2)
        def _():
            convolve(stage - 2)
            for shift in range(1, levels):
                spread(level, stage - 2, shift, lax.rem(level + shift, levels)).start()
            score(level, stage - 2)

    @pl.loop(0, blocks)
    def _(order):
        for shift in range(1, levels):
            sender = lax.rem(level + levels - shift, levels)
            spread(sender, order, shift, sender).wait_recv()
            score(sender, order)

    for way in range(2):
        pl.when(has[way])(lambda: halo(way).wait_send())
    for shift in range(1, levels):
        table_out(shift).wait_send()
        for kind in range(3):
            over_level(kind, shift).wait_send()

    @pl.loop(0, blocks)
    def _(order):
        for shift in range(1, levels):
            spread(level, order, shift, lax.rem(level + shift, levels)).wait_send()


def decode_step(levels, devices, ids, fill, table, w_qkv, w_out_t, w_expand, w_project, head, taps):
    frames, width = ids.shape[0], table.shape[1]
    chips = devices // CORES
    local_rows = frames // levels
    blocks = local_rows // math.gcd(local_rows, 2 * LANES)
    span = max(frames, width)
    meta = jnp.concatenate(
        [
            jnp.broadcast_to(jnp.pad(ids, (0, span - frames)), (8, span)),
            jnp.broadcast_to(jnp.pad(fill, (0, span - width)), (8, span)),
        ]
    )
    vmem = pl.BlockSpec(memory_space=pltpu.VMEM)
    anywhere = pl.BlockSpec(memory_space=pl.ANY)
    dma = pltpu.SemaphoreType.DMA
    half = chips // 2
    bf16, f32 = jnp.bfloat16, jnp.float32
    return pl.pallas_call(
        functools.partial(step_kernel, levels, devices, frames, width),
        out_shape=jax.ShapeDtypeStruct((frames, head.shape[1]), bf16),
        in_specs=[anywhere] * 7 + [vmem],
        out_specs=vmem,
        scratch_shapes=[
            pltpu.VMEM((levels,) + meta.shape, f32),
            pltpu.VMEM((levels,) + table.shape, bf16),
            pltpu.VMEM((3, width, width), bf16),
            pltpu.VMEM((4, width, width), bf16),
            pltpu.VMEM((frames, width), f32),
            pltpu.VMEM((frames, width), bf16),
            pltpu.VMEM((frames, width), bf16),
            pltpu.VMEM((frames, width), bf16),
            pltpu.VMEM((local_rows, width), bf16),
            pltpu.VMEM((local_rows, width), bf16),
            pltpu.VMEM((local_rows + 2 * HALO, width), bf16),
            pltpu.VMEM((frames, width), bf16),
            pltpu.VMEM(head.shape, bf16),
            dma((2,)), dma((2,)), dma((blocks, levels)), dma((blocks, levels)),
            dma((8,)),
            dma((3, levels)), dma((3, levels)), dma((2, levels)), dma((2, levels)),
        ]
        + [dma((2, half)), dma((2, half)), dma((2, half + 1)), dma((2, half + 1))] * 2,
        compiler_params=pltpu.CompilerParams(
            collective_id=0, has_side_effects=True, vmem_limit_bytes=64000 * 1024
        ),
    )(meta, table, w_qkv, w_out_t, w_expand, w_project, head, taps)


def body(
    token_ids,
    decoded_mask,
    levels_done,
    code_tables,
    mask_vectors,
    w_qkv,
    w_out,
    w_expand,
    w_depth,
    w_project,
    level_heads,
):
    groups = lax.axis_size("level")
    level_index = lax.axis_index("level")
    done_count = levels_done[0]
    use_token = (level_index < done_count) | ((level_index == done_count) & (decoded_mask[0, 0] == 1))
    ids = jnp.where(use_token, token_ids[0, 0], -1).astype(jnp.float32)
    logits = decode_step(
        groups, lax.axis_size("dp"), ids, mask_vectors[0].astype(jnp.float32), code_tables[0],
        w_qkv, w_out.T[None], w_expand, w_project, level_heads[0], w_depth.astype(jnp.float32),
    )
    return logits[None, None]


def solution(mesh):
    return jax.shard_map(
        body,
        mesh=mesh,
        in_specs=(
            P("dp", "level", None),
            P("dp", "level", None),
            P("dp"),
            P("level", None, None),
            P("level", None),
            P(None, "dp", "level"),
            P("level", "dp"),
            P("dp", None),
            P(),
            P("dp", None),
            P("level", None, None),
        ),
        out_specs=P("dp", "level", None, None),
        check_vma=False,
    )
```

```python
import functools
import math

import jax
import jax.numpy as jnp
from jax import lax
from jax.experimental import pallas as pl
from jax.experimental.pallas import tpu as pltpu
from jax.sharding import PartitionSpec as P

HEADS = 16
CORES = 2
LANES = 128
HALO = 16
MESH = pl.DeviceIdType.MESH


def layer_norm(values):
    centered = values - jnp.mean(values, axis=-1, keepdims=True)
    variance = jnp.mean(centered * centered, axis=-1, keepdims=True)
    return centered * lax.rsqrt(variance + 1e-05)


def dot_f32(left, right):
    return jnp.dot(left, right, preferred_element_type=jnp.float32)


def dot_nt(left, right):
    return lax.dot_general(left, right, (((1,), (1,)), ((), ())), preferred_element_type=jnp.float32)


def chip_at(position, chips):
    position = lax.rem(position + 2 * chips, chips)
    turned = position // (chips // 2)
    return (1 - turned) * 2 * position + turned * (2 * (chips - 1 - position) + 1)


def position_of(chip, chips):
    odd = lax.rem(chip, 2)
    return (1 - odd) * (chip // 2) + odd * (chips - 1 - chip // 2)


class Ring:
    def __init__(self, full, rows, chips, sems):
        self.full, self.rows, self.chips, self.half = full, rows, chips, chips // 2
        self.send, self.recv, self.sib_send, self.sib_recv = sems
        self.device = lax.axis_index("dp")
        self.core = lax.rem(self.device, CORES)
        self.position = position_of(self.device // CORES, chips)
        self.sent = []

    def block(self, position, core, part):
        row = (chip_at(position, self.chips) * CORES + core) * self.rows
        count = self.rows
        if part is not None:
            count = self.rows // 2
            row = row + part * count
        return self.full.at[:, pl.ds(pl.multiple_of(row, count), count), :]

    def part(self, way, step):
        return way if step == self.half - 1 else None

    def origin(self, way, step):
        return self.position - (1 + step) if way == 0 else self.position + (1 + step)

    def hop(self, way, step):
        towards = self.position + 1 if way == 0 else self.position - 1
        source = self.position - step if way == 0 else self.position + step
        ref = self.block(source, self.core, self.part(way, step))
        target = chip_at(towards, self.chips) * CORES + self.core
        return pltpu.make_async_remote_copy(
            src_ref=ref,
            dst_ref=ref,
            send_sem=self.send.at[way, step],
            recv_sem=self.recv.at[way, step],
            device_id={"dp": target},
            device_id_type=MESH,
        )

    def arrival(self, way, step):
        ref = self.block(self.origin(way, step), self.core, self.part(way, step))
        return pltpu.make_async_remote_copy(
            src_ref=ref,
            dst_ref=ref,
            send_sem=self.send.at[way, step],
            recv_sem=self.recv.at[way, step],
            device_id={"dp": self.device},
            device_id_type=MESH,
        )

    def share(self, way, step, core):
        position = self.position if step < 0 else self.origin(way, step)
        ref = self.block(position, core, None if step < 0 else self.part(way, step))
        sibling = self.device + 1 - 2 * self.core
        return pltpu.make_async_remote_copy(
            src_ref=ref,
            dst_ref=ref,
            send_sem=self.sib_send.at[way, step + 1],
            recv_sem=self.sib_recv.at[way, step + 1],
            device_id={"dp": sibling},
            device_id_type=MESH,
        )

    def start(self):
        for way in range(2):
            self.hop(way, 0).start()
        self.share(0, -1, self.core).start()

    def advance(self, step):
        for way in range(2):
            self.arrival(way, step).wait_recv()
            if step + 1 < self.half:
                self.hop(way, step + 1).start()
            self.share(way, step, self.core).start()

    def finish(self):
        for way in range(2):
            for step in range(self.half):
                self.hop(way, step).wait_send()
                self.share(way, step, self.core).wait_send()
                self.share(way, step, 1 - self.core).wait_recv()
        self.share(0, -1, self.core).wait_send()
        self.share(0, -1, 1 - self.core).wait_recv()


def step_kernel(
    levels, devices, frames, width,
    meta_ref, table_ref, qkv_ref, out_ref, expand_ref, project_ref, head_ref, depth_ref,
    logits_ref,
    metas, tables, proj, rest_ref, embedded, normed, keys, values, queries,
    attended, gated, final, head,
    halo_send, halo_recv, final_send, final_recv,
    local_sem, level_send, level_recv, table_send, table_recv,
    ring_a, ring_a_recv, sib_a, sib_a_recv, ring_b, ring_b_recv, sib_b, sib_b_recv,
):
    level = lax.axis_index("level")
    device = lax.axis_index("dp")
    core = lax.rem(device, CORES)
    sibling = device + 1 - 2 * core
    chips = devices // CORES
    rows = width // devices
    columns = width // levels
    local_rows = frames // levels
    codes = table_ref.shape[0]
    half_table = codes // CORES
    position = position_of(device // CORES, chips)

    barrier = pltpu.get_barrier_semaphore()
    for shift in range(1, levels):
        pl.semaphore_signal(barrier, inc=1, device_id={"level": lax.rem(level + shift, levels)}, device_id_type=MESH)
    for other in (
        sibling,
        chip_at(position + 1, chips) * CORES + core,
        chip_at(position - 1, chips) * CORES + core,
    ):
        pl.semaphore_signal(barrier, inc=1, device_id={"dp": other}, device_id_type=MESH)
    pl.semaphore_wait(barrier, levels + 2)

    own_rows = pl.ds(pl.multiple_of(device * rows, rows), rows)
    own_columns = pl.ds(pl.multiple_of(level * columns, columns), columns)
    places = (
        (qkv_ref, proj.at[:, own_rows, own_columns]),
        (out_ref, rest_ref.at[pl.ds(0, 1), own_rows, own_columns]),
        (meta_ref, metas.at[level]),
    )
    half_rows = pl.ds(pl.multiple_of(core * half_table, half_table), half_table)
    other_half = pl.ds(pl.multiple_of((1 - core) * half_table, half_table), half_table)

    def over_level(kind, shift):
        source, place = places[kind]
        return pltpu.make_async_remote_copy(
            src_ref=source, dst_ref=place,
            send_sem=level_send.at[kind, shift], recv_sem=level_recv.at[kind, shift],
            device_id={"level": lax.rem(level + shift, levels)}, device_id_type=MESH,
        )

    def from_level(kind, shift):
        sender = lax.rem(level + levels - shift, levels)
        sender_columns = pl.ds(pl.multiple_of(sender * columns, columns), columns)
        source = places[kind][0]
        place = (
            proj.at[:, own_rows, sender_columns],
            rest_ref.at[pl.ds(0, 1), own_rows, sender_columns],
            metas.at[sender],
        )[kind]
        return pltpu.make_async_remote_copy(
            src_ref=source, dst_ref=place,
            send_sem=level_send.at[kind, shift], recv_sem=level_recv.at[kind, shift],
            device_id={"level": sender}, device_id_type=MESH,
        )

    def table_out(shift):
        return pltpu.make_async_remote_copy(
            src_ref=table_ref.at[half_rows], dst_ref=tables.at[level, half_rows],
            send_sem=table_send.at[0, shift], recv_sem=table_recv.at[0, shift],
            device_id={"level": lax.rem(level + shift, levels)}, device_id_type=MESH,
        )

    def table_at(shift, span, kind):
        sender = lax.rem(level + levels - shift, levels)
        place = tables.at[sender, span]
        return pltpu.make_async_remote_copy(
            src_ref=place, dst_ref=place,
            send_sem=table_send.at[kind, shift], recv_sem=table_recv.at[kind, shift],
            device_id={"dp": sibling}, device_id_type=MESH,
        )

    locals_ = [
        pltpu.make_async_copy(source, place, local_sem.at[i]) for i, (source, place) in enumerate(places)
    ] + [
        pltpu.make_async_copy(table_ref, tables.at[level], local_sem.at[3]),
        pltpu.make_async_copy(expand_ref.at[:, pl.ds(0, width)], rest_ref.at[1, own_rows, :], local_sem.at[4]),
        pltpu.make_async_copy(expand_ref.at[:, pl.ds(width, width)], rest_ref.at[2, own_rows, :], local_sem.at[5]),
        pltpu.make_async_copy(project_ref, rest_ref.at[3, own_rows, :], local_sem.at[6]),
    ]
    head_copy = pltpu.make_async_copy(head_ref, head, local_sem.at[7])
    for kind in (0, 2):
        for shift in range(1, levels):
            over_level(kind, shift).start()
    for copy in locals_:
        copy.start()
    for shift in range(1, levels):
        table_out(shift).start()
    for shift in range(1, levels):
        over_level(1, shift).start()
    head_copy.start()

    def rings(full, count, sems):
        return [
            Ring(full.at[pl.ds(piece, 1)], rows, chips, tuple(sem.at[piece] for sem in sems))
            for piece in range(count)
        ]

    first = rings(proj, 3, (ring_a, ring_a_recv, sib_a, sib_a_recv))
    second = rings(rest_ref, 4, (ring_b, ring_b_recv, sib_b, sib_b_recv))

    for copy in locals_:
        copy.wait()
    for shift in range(1, levels):
        from_level(0, shift).wait_recv()
    hops = chips // 2
    for ring in first:
        ring.start()
    for step in range(hops - 1):
        for ring in first:
            ring.advance(step)
    for shift in range(1, levels):
        from_level(1, shift).wait_recv()
    for ring in second:
        ring.start()
    for shift in range(1, levels):
        from_level(2, shift).wait_recv()
        table_at(shift, half_rows, 0).wait_recv()
        table_at(shift, half_rows, 1).start()
    for shift in range(1, levels):
        table_at(shift, half_rows, 1).wait_send()
        table_at(shift, other_half, 1).wait_recv()

    tile = 2 * LANES
    @pl.loop(0, frames // tile)
    def _(step):
        for piece, ring in enumerate(first):
            @pl.when(step == min(2 + piece, frames // tile - 1))
            def _():
                ring.advance(hops - 1)

        span = pl.ds(pl.multiple_of(step * tile, tile), tile)
        total = jnp.zeros((tile, width), jnp.float32)
        lane = lax.broadcasted_iota(jnp.int32, (tile, LANES), 1).astype(jnp.float32)
        for row in range(levels):
            ids = jnp.concatenate(
                [
                    jnp.broadcast_to(
                        metas[row, 0:1, pl.ds(pl.multiple_of(step * tile + piece * LANES, LANES), LANES)],
                        (LANES, LANES),
                    ).T
                    for piece in range(tile // LANES)
                ],
                axis=0,
            )
            onehot = jnp.concatenate(
                [
                    jnp.where(ids == lane + float(base), 1.0, 0.0).astype(jnp.bfloat16)
                    for base in range(0, codes, LANES)
                ],
                axis=1,
            )
            picked = dot_f32(onehot, tables[row])
            fill = metas[row, 8:9, 0:width]
            total = total + jnp.where(ids[:, 0:1] < 0.0, fill, picked)
        embedded[span, :] = total
        normed[span, :] = layer_norm(total).astype(jnp.bfloat16)

    for ring in first:
        ring.finish()

    @pl.loop(0, frames // tile)
    def _(step):
        for piece, ring in enumerate(second):
            @pl.when(step == min(2 + piece, frames // tile - 1))
            def _():
                ring.advance(0)

        span = pl.ds(pl.multiple_of(step * tile, tile), tile)
        keys[span, :] = dot_f32(normed[span, :], proj[1]).astype(jnp.bfloat16)
        values[span, :] = dot_f32(normed[span, :], proj[2]).astype(jnp.bfloat16)

    head_dim = width // HEADS
    scale = head_dim ** (-0.5)
    block = math.gcd(local_rows, tile)

    @pl.loop(0, local_rows // block)
    def _(step):
        begin = pl.multiple_of(level * local_rows + step * block, block)
        to = pl.ds(pl.multiple_of(step * block, block), block)
        found = dot_f32(normed[pl.ds(begin, block), :], proj[0]).astype(jnp.bfloat16)
        queries[to, :] = found * jnp.asarray(scale, jnp.bfloat16)

    blocks = local_rows // block
    pairs = width // LANES
    turns = pairs * min(2, blocks)
    events = [(step, ring) for step in range(1, hops) for ring in second]
    pad = HALO
    taps = depth_ref.shape[0]
    odd_level = lax.rem(level, 2)

    def chunk_of(owner, order):
        odd = lax.rem(owner, 2)
        return odd * order + (1 - odd) * (blocks - 1 - order)

    def local_span(order):
        return pl.ds(pl.multiple_of(chunk_of(level, order) * block, block), block)

    def clip_span(owner, order):
        start = owner * local_rows + chunk_of(owner, order) * block
        return pl.ds(pl.multiple_of(start, block), block)

    def halo(way):
        source = (pl.ds(local_rows, pad), pl.ds(pad, pad))[way]
        place = (pl.ds(0, pad), pl.ds(pad + local_rows, pad))[way]
        target = level + 1 if way == 0 else level - 1
        return pltpu.make_async_remote_copy(
            src_ref=gated.at[source], dst_ref=gated.at[place],
            send_sem=halo_send.at[way], recv_sem=halo_recv.at[way],
            device_id={"level": target}, device_id_type=MESH,
        )

    has = (level < levels - 1, level > 0)

    def halo_start(way):
        pl.when(has[way])(lambda: halo(way).start())

    def halo_wait(way):
        pl.when(has[1 - way])(lambda: halo(way).wait_recv())

    def spread(owner, order, shift, target):
        return pltpu.make_async_remote_copy(
            src_ref=final.at[clip_span(owner, order)], dst_ref=final.at[clip_span(owner, order)],
            send_sem=final_send.at[order, shift], recv_sem=final_recv.at[order, shift],
            device_id={"level": target}, device_id_type=MESH,
        )

    @pl.when(level == 0)
    def _():
        gated[pl.ds(0, pad), :] = jnp.zeros((pad, width), jnp.bfloat16)

    @pl.when(level == levels - 1)
    def _():
        gated[pl.ds(pad + local_rows, pad), :] = jnp.zeros((pad, width), jnp.bfloat16)

    def attend(order):
        to = local_span(order)

        @pl.loop(0, pairs)
        def _(pair):
            turn = order * pairs + pair
            for event, (step, ring) in enumerate(events):
                @pl.when(turn == event * turns // len(events))
                def _():
                    ring.advance(step)

            across = pl.ds(pl.multiple_of(pair * LANES, LANES), LANES)
            query = queries[to, across]
            key = keys[:, across]
            value = values[:, across]
            lower = lax.broadcasted_iota(jnp.int32, (block, LANES), 1) < head_dim
            lower_value = lax.broadcasted_iota(jnp.int32, (frames, LANES), 1) < head_dim
            one = jnp.ones_like(value)
            zero = jnp.zeros_like(query)
            sums = []
            for low in (True, False):
                masked = jnp.where(lower, query, zero) if low else jnp.where(lower, zero, query)
                scores = dot_nt(masked, key)
                weights = jnp.exp(scores - jnp.max(scores, axis=-1, keepdims=True)).astype(jnp.bfloat16)
                extended = jnp.where(lower_value, value, one) if low else jnp.where(lower_value, one, value)
                sums.append(dot_f32(weights, extended))
            above = jnp.where(lower, sums[0], sums[1])
            below = pltpu.roll(jnp.where(lower, sums[1], sums[0]), head_dim, 1)
            attended[to, across] = (above / below).astype(jnp.bfloat16)

    def gate(order):
        own = clip_span(level, order)
        after_attn = embedded[own, :] + dot_nt(attended[local_span(order), :], rest_ref[0])
        embedded[own, :] = after_attn
        normed_two = layer_norm(after_attn).astype(jnp.bfloat16)
        mixed = dot_f32(normed_two, rest_ref[1]) * jax.nn.sigmoid(dot_f32(normed_two, rest_ref[2]))
        start = pl.multiple_of(pad + chunk_of(level, order) * block, pad)
        gated[pl.ds(start, block), :] = mixed.astype(jnp.bfloat16)

    def convolve(order):
        own = clip_span(level, order)
        start = pl.multiple_of(chunk_of(level, order) * block, block)
        window = gated[pl.ds(start, block + 2 * pad), :].astype(jnp.float32)
        conv = jnp.zeros((block, width), jnp.float32)
        for tap in range(taps):
            first_row = pad - taps // 2 + tap
            conv = conv + window[first_row : first_row + block] * depth_ref[tap : tap + 1, :]
        activated = (conv * jax.nn.sigmoid(conv)).astype(jnp.bfloat16)
        after_conv = embedded[own, :] + dot_f32(activated, rest_ref[3])
        final[own, :] = layer_norm(after_conv).astype(jnp.bfloat16)

    def score(owner, order):
        span = clip_span(owner, order)
        logits_ref[span, :] = dot_f32(final[span, :], head[...]).astype(jnp.bfloat16)

    def send_and_score(order):
        convolve(order)
        for shift in range(1, levels):
            spread(level, order, shift, lax.rem(level + shift, levels)).start()
        score(level, order)

    def by_parity(act, even_way):
        pl.when(odd_level == 0)(lambda: act(even_way))
        pl.when(odd_level == 1)(lambda: act(1 - even_way))

    @pl.loop(0, blocks)
    def _(stage):
        attend(stage)

        @pl.when(stage == 1)
        def _():
            for ring in second:
                ring.finish()
            head_copy.wait()
            gate(0)
            by_parity(halo_start, 0)

        @pl.when(stage >= 1)
        def _():
            gate(stage)

        @pl.when(stage == blocks - 1)
        def _():
            by_parity(halo_start, 1)

        @pl.when(stage == 1)
        def _():
            by_parity(halo_wait, 1)

        @pl.when(stage >= 1)
        def _():
            send_and_score(stage - 1)

    by_parity(halo_wait, 0)
    send_and_score(blocks - 1)

    @pl.loop(0, blocks)
    def _(order):
        for shift in range(1, levels):
            sender = lax.rem(level + levels - shift, levels)
            spread(sender, order, shift, sender).wait_recv()
            score(sender, order)

    for way in range(2):
        pl.when(has[way])(lambda: halo(way).wait_send())
    for shift in range(1, levels):
        table_out(shift).wait_send()
        for kind in range(3):
            over_level(kind, shift).wait_send()

    @pl.loop(0, blocks)
    def _(order):
        for shift in range(1, levels):
            spread(level, order, shift, lax.rem(level + shift, levels)).wait_send()


def decode_step(levels, devices, ids, fill, table, w_qkv, w_out_t, w_expand, w_project, head, taps):
    frames, width = ids.shape[0], table.shape[1]
    chips = devices // CORES
    local_rows = frames // levels
    blocks = local_rows // math.gcd(local_rows, 2 * LANES)
    span = max(frames, width)
    meta = jnp.concatenate(
        [
            jnp.broadcast_to(jnp.pad(ids, (0, span - frames)), (8, span)),
            jnp.broadcast_to(jnp.pad(fill, (0, span - width)), (8, span)),
        ]
    )
    vmem = pl.BlockSpec(memory_space=pltpu.VMEM)
    anywhere = pl.BlockSpec(memory_space=pl.ANY)
    dma = pltpu.SemaphoreType.DMA
    half = chips // 2
    bf16, f32 = jnp.bfloat16, jnp.float32
    return pl.pallas_call(
        functools.partial(step_kernel, levels, devices, frames, width),
        out_shape=jax.ShapeDtypeStruct((frames, head.shape[1]), bf16),
        in_specs=[anywhere] * 7 + [vmem],
        out_specs=vmem,
        scratch_shapes=[
            pltpu.VMEM((levels,) + meta.shape, f32),
            pltpu.VMEM((levels,) + table.shape, bf16),
            pltpu.VMEM((3, width, width), bf16),
            pltpu.VMEM((4, width, width), bf16),
            pltpu.VMEM((frames, width), f32),
            pltpu.VMEM((frames, width), bf16),
            pltpu.VMEM((frames, width), bf16),
            pltpu.VMEM((frames, width), bf16),
            pltpu.VMEM((local_rows, width), bf16),
            pltpu.VMEM((local_rows, width), bf16),
            pltpu.VMEM((local_rows + 2 * HALO, width), bf16),
            pltpu.VMEM((frames, width), bf16),
            pltpu.VMEM(head.shape, bf16),
            dma((2,)), dma((2,)), dma((blocks, levels)), dma((blocks, levels)),
            dma((8,)),
            dma((3, levels)), dma((3, levels)), dma((2, levels)), dma((2, levels)),
        ]
        + [
            dma((count, 2, half + extra)) for count in (3, 4) for extra in (0, 0, 1, 1)
        ],
        compiler_params=pltpu.CompilerParams(
            collective_id=0, has_side_effects=True, vmem_limit_bytes=64000 * 1024
        ),
    )(meta, table, w_qkv, w_out_t, w_expand, w_project, head, taps)


def body(
    token_ids,
    decoded_mask,
    levels_done,
    code_tables,
    mask_vectors,
    w_qkv,
    w_out,
    w_expand,
    w_depth,
    w_project,
    level_heads,
):
    groups = lax.axis_size("level")
    level_index = lax.axis_index("level")
    done_count = levels_done[0]
    use_token = (level_index < done_count) | ((level_index == done_count) & (decoded_mask[0, 0] == 1))
    ids = jnp.where(use_token, token_ids[0, 0], -1).astype(jnp.float32)
    logits = decode_step(
        groups, lax.axis_size("dp"), ids, mask_vectors[0].astype(jnp.float32), code_tables[0],
        w_qkv, w_out.T[None], w_expand, w_project, level_heads[0], w_depth.astype(jnp.float32),
    )
    return logits[None, None]


def solution(mesh):
    return jax.shard_map(
        body,
        mesh=mesh,
        in_specs=(
            P("dp", "level", None),
            P("dp", "level", None),
            P("dp"),
            P("level", None, None),
            P("level", None),
            P(None, "dp", "level"),
            P("level", "dp"),
            P("dp", None),
            P(),
            P("dp", None),
            P("level", None, None),
        ),
        out_specs=P("dp", "level", None, None),
        check_vma=False,
    )
```
